32 devices in a mesh: dp: 2 (over z, core), sp: 16 (over x, y).
Axes of the slice: x: 4, y: 4, z: 1, core: 2. Of those that a mesh axis runs over, the one named last changes fastest.
The devices are a block of a 4x4x8 slice.
Arguments:
- x: bfloat16 [8192, 2048], P(('dp', 'sp')), parts along dimension 0
- gain: bfloat16 [2048], replicated
- wq: bfloat16 [2048, 4096], replicated
- wk: bfloat16 [2048, 512], replicated
- wv: bfloat16 [2048, 512], replicated
- wo: bfloat16 [4096, 2048], replicated
Outputs:
- output: bfloat16 [8192, 2048], P(('dp', 'sp')), parts along dimension 0
There are 2 independent parts. The reference program is written for one: setup_inputs(seed, part) draws one part's arguments, and reference() takes and returns one part's arrays. A program takes and returns all parts, laid end to end along the dimension named above; an argument that names none is the same for every part.
All inputs are finite; a program needn't handle non-finite values.
Results may differ from the reference program's by a relative error of at most 0.012.
Values are sent between devices in bfloat16 or wider.
A program may use at most 768 MiB of HBM per device.

```python
import jax
import jax.numpy as jnp
from jax import lax

ROWS = 4096
D = 2048
HEADS = 16
KV_HEADS = 2
HEAD = 256
THETA = 10000


def setup_inputs(seed: int = 0, part: int = 0) -> dict:
    kx, kn, kq, kk, kv, ko = jax.random.split(jax.random.key(seed), 6)

    def weights(key, rows, columns):
        return jax.random.normal(key, (rows, columns), jnp.float32) * rows**-0.5

    drawn = {
        "x": jax.random.normal(jax.random.fold_in(kx, part), (ROWS, D), jnp.float32),
        "gain": 1 + 0.1 * jax.random.normal(kn, (D,), jnp.float32),
        "wq": 2 * weights(kq, D, HEADS * HEAD),
        "wk": 2 * weights(kk, D, KV_HEADS * HEAD),
        "wv": 4 * weights(kv, D, KV_HEADS * HEAD),
        "wo": weights(ko, HEADS * HEAD, D),
    }
    return {k: v.astype(jnp.bfloat16) for k, v in drawn.items()}


def normed(x, gain):
    wide = x.astype(jnp.float32)
    scale = lax.rsqrt(jnp.mean(wide * wide, -1, keepdims=True) + 1e-6)
    return (wide * scale * gain.astype(jnp.float32)).astype(jnp.bfloat16)


def turned(t, place, theta):
    half = t.shape[-1] // 2
    angle = place.astype(jnp.float32)[:, None] * theta ** (-jnp.arange(half, dtype=jnp.float32) / half)
    cos, sin = jnp.cos(angle)[:, None], jnp.sin(angle)[:, None]
    a, b = t[..., :half].astype(jnp.float32), t[..., half:].astype(jnp.float32)
    return jnp.concatenate([a * cos - b * sin, b * cos + a * sin], -1).astype(jnp.bfloat16)


def matmul(a, w):
    return jnp.dot(a, w, preferred_element_type=jnp.float32).astype(jnp.bfloat16)


def einsum(form, a, b):
    return jnp.einsum(form, a.astype(jnp.float32), b.astype(jnp.float32))


def attention(q, k, v):
    scores = einsum("tgsd,ugd->gstu", q, k) * q.shape[-1] ** -0.5
    token = jnp.arange(q.shape[0])
    scores = jnp.where(token[:, None] >= token, scores, -jnp.inf)
    weights = jax.nn.softmax(scores, -1).astype(jnp.bfloat16)
    return einsum("gstu,ugd->tgsd", weights, v).astype(jnp.bfloat16)


def reference(x, gain, wq, wk, wv, wo):
    a, place = normed(x, gain), jnp.arange(ROWS)
    q = turned(matmul(a, wq).reshape(ROWS, HEADS, HEAD), place, THETA).reshape(ROWS, KV_HEADS, -1, HEAD)
    k = turned(matmul(a, wk).reshape(ROWS, KV_HEADS, HEAD), place, THETA)
    v = matmul(a, wv).reshape(ROWS, KV_HEADS, HEAD)
    seen = attention(q, k, v).reshape(ROWS, HEADS * HEAD)
    return (x.astype(jnp.float32) + jnp.dot(seen, wo, preferred_element_type=jnp.float32)).astype(jnp.bfloat16)
```

```python
import functools
import math

import jax
import jax.numpy as jnp
import numpy as np
from jax import lax
from jax.experimental import pallas as pl
from jax.experimental.pallas import tpu as pltpu
from jax.sharding import PartitionSpec as P

HEAD = 256
THETA = 10000
LOG2E = 1.4426950408889634
HIDDEN = -2e30
STRIP = 512
MESH = pl.DeviceIdType.MESH


def dot(a, b, ca, cb):
    return lax.dot_general(a, b, (((ca,), (cb,)), ((), ())), preferred_element_type=jnp.float32)


def kernel(n, x_hbm, gain_ref, freq_ref, wq_hbm, wk_hbm, wv_hbm, wo_hbm, y_hbm, x_s, wk_s, wv_s, w_s, a_s, cos_s, sin_s, q_s, kv_s, top_s, mix_s, o_s, y_s,
           x_sem, wk_sem, wv_sem, w_sem, y_sem, send_sem, recv_sem):
    side = math.isqrt(n)
    own, width = x_s.shape
    half = HEAD // 2
    kvh = kv_s.shape[1]
    chunks, _, wide = w_s.shape
    heads = wq_hbm.shape[1] // HEAD
    group = heads // kvh
    cols = group * own
    me = lax.axis_index("sp")
    mx, my = me // side, me % side
    turn = (mx + my) % side
    place = (mx * side + turn, my * side + turn)

    def device(cycle, p):
        p = (p + n) % n
        major = p // side
        minor = (p % side + (side - 1) * major) % side
        return major * side + minor if cycle == 0 else minor * side + major

    neighbour = {(c, d): device(c, place[c] + (1 if d == 0 else -1)) for c in range(2) for d in range(2)}

    def source(c, d, t):
        return device(c, place[c] - t if d == 0 else place[c] + t)

    def copy(c, d, t, sub):
        block = kv_s.at[source(c, d, t), c, sub]
        return pltpu.make_async_remote_copy(src_ref=block, dst_ref=block, send_sem=send_sem.at[c, d, t, sub], recv_sem=recv_sem.at[c, d, t, sub],
                                            device_id={"sp": neighbour[c, d]}, device_id_type=MESH)

    def arrived(c, d, t, sub):
        block = kv_s.at[source(c, d, t), c, sub]
        pltpu.make_async_remote_copy(src_ref=block, dst_ref=block, send_sem=send_sem.at[c, d, t - 1, sub], recv_sem=recv_sem.at[c, d, t - 1, sub],
                                     device_id={"sp": neighbour[c, d]}, device_id_type=MESH).wait_recv()

    x_copy = pltpu.make_async_copy(x_hbm, x_s, x_sem)
    wk_copy = pltpu.make_async_copy(wk_hbm, wk_s, wk_sem)
    wv_copy = pltpu.make_async_copy(wv_hbm, wv_s, wv_sem)
    x_copy.start()
    wk_copy.start()
    wv_copy.start()

    barrier = pltpu.get_barrier_semaphore()
    for c in range(2):
        for d in range(2):
            pl.semaphore_signal(barrier, inc=1, device_id={"sp": neighbour[c, d]}, device_id_type=MESH)

    angle = (me * own + lax.broadcasted_iota(jnp.int32, (own, half), 0)).astype(jnp.float32) * freq_ref[...]
    cos_s[...] = jnp.cos(angle)
    sin_s[...] = jnp.sin(angle)

    def turned(t):
        a, b = t[:, :half], t[:, half:]
        return jnp.concatenate([a * cos_s[...] - b * sin_s[...], b * cos_s[...] + a * sin_s[...]], 1).astype(jnp.bfloat16)

    def rounded(t):
        return t.astype(jnp.bfloat16).astype(jnp.float32)

    x_copy.wait()
    rows = 32

    def norm(i, _):
        at = pl.ds(pl.multiple_of(i * rows, rows), rows)
        t = x_s[at, :].astype(jnp.float32)
        scale = lax.rsqrt(jnp.mean(t * t, -1, keepdims=True) + 1e-6)
        a_s[at, :] = (t * scale * gain_ref[...].astype(jnp.float32)).astype(jnp.bfloat16)
        return _

    lax.fori_loop(0, own // rows, norm, 0)

    wk_copy.wait()
    keys = rounded(dot(a_s[...], wk_s[...], 1, 0))
    for c in range(kvh):
        kv_s[me, c, 0] = turned(keys[:, c * HEAD : (c + 1) * HEAD])
    wv_copy.wait()

    def wq_copy(i):
        return pltpu.make_async_copy(wq_hbm.at[:, pl.ds(pl.multiple_of(i * wide, wide), wide)], w_s.at[i], w_sem.at[i])

    for i in range(chunks):
        wq_copy(i).start()
    pl.semaphore_wait(barrier, 4)
    for c in range(2):
        for d in range(2):
            copy(c, d, 0, 0).start()
    values = dot(a_s[...], wv_s[...], 1, 0).astype(jnp.bfloat16)
    for c in range(kvh):
        kv_s[me, c, 1] = values[:, c * HEAD : (c + 1) * HEAD].T
    per = wide // HEAD

    def project(i, _):
        wq_copy(i).wait()
        for j in range(per):
            t = rounded(dot(a_s[...], w_s[i, :, j * HEAD : (j + 1) * HEAD], 1, 0))
            h = i * per + j
            q_s[h // group, pl.ds(pl.multiple_of((h % group) * own, own), own), :] = turned(t)
        return _

    lax.fori_loop(0, 1, project, 0)
    for c in range(2):
        for d in range(2):
            copy(c, d, 0, 1).start()
    e = HEAD**-0.5 * LOG2E
    ones = jnp.ones((8, own), jnp.bfloat16)

    def unit(slot, c, first):
        for at in range(0, cols, STRIP):
            strip = slice(at, at + STRIP)
            s = dot(kv_s[slot, c, 0], q_s[c, strip, :], 1, 1)
            if first:
                query = lax.broadcasted_iota(jnp.int32, (own, STRIP), 1) % own
                s = jnp.where(query >= lax.broadcasted_iota(jnp.int32, (own, STRIP), 0), s, HIDDEN)
            top = s.max(axis=0, keepdims=True)
            if not first:
                old = top_s[c, :, strip]
                top = jnp.maximum(old, top)
            top_s[c, :, strip] = top
            p = jnp.exp2((s - top) * e).astype(jnp.bfloat16)
            add = dot(jnp.concatenate([kv_s[slot, c, 1], ones], axis=0), p, 1, 0)
            mix_s[c, :, strip] = add if first else mix_s[c, :, strip] * jnp.exp2((old - top) * e) + add

    def units(c, t):
        for d in range(2):
            slot = source(c, d, t)

            @pl.when(slot < me)
            def _():
                unit(slot, c, False)

    def hand_on(t, sub, last):
        for c in range(2):
            for d in range(2):
                arrived(c, d, t, sub)
                if last is None or d == last:
                    copy(c, d, t, sub).start()

    lax.fori_loop(1, chunks - 1, project, 0)
    hand_on(1, 0, None)
    lax.fori_loop(chunks - 1, chunks, project, 0)

    def wo_copy(i):
        r, j = i % 2, i // 2
        rows = w_s.shape[1]
        return pltpu.make_async_copy(wo_hbm.at[pl.ds(r * rows, rows), pl.ds(j * wide, wide)], w_s.at[i], w_sem.at[i])

    for i in range(chunks):
        wo_copy(i).start()
    for c in range(kvh):
        unit(me, c, True)
    hand_on(1, 1, None)
    units(0, 1)
    middle = n // 2

    def step(t, _):
        hand_on(t, 0, None)
        units(1, t - 1)
        hand_on(t, 1, None)
        units(0, t)
        return _

    lax.fori_loop(2, middle - 1, step, 0)
    hand_on(middle - 1, 0, 0)
    units(1, middle - 2)
    hand_on(middle - 1, 1, 1)
    units(0, middle - 1)
    units(1, middle - 1)
    for c in range(2):
        arrived(c, 0, middle, 0)
        arrived(c, 1, middle, 1)
        slot = source(c, 0, middle)

        @pl.when(slot < me)
        def _():
            unit(slot, c, False)

    for c in range(kvh):
        for j in range(group):
            at = slice(j * own, (j + 1) * own)
            out = mix_s[c, :HEAD, at] * (1 / mix_s[c, HEAD : HEAD + 1, at])
            o_s[:, (c * group + j) * HEAD : (c * group + j + 1) * HEAD] = out.astype(jnp.bfloat16).T
    k = w_s.shape[1]
    for j in range(chunks // 2):
        at = slice(j * wide, (j + 1) * wide)
        wo_copy(2 * j).wait()
        wo_copy(2 * j + 1).wait()
        y = dot(o_s[:, :k], w_s[2 * j], 1, 0) + dot(o_s[:, k:], w_s[2 * j + 1], 1, 0)
        y_s[:, at] = (x_s[:, at].astype(jnp.float32) + y).astype(jnp.bfloat16)
        pltpu.make_async_copy(y_s.at[:, at], y_hbm.at[:, at], y_sem.at[j]).start()

    def sent(t, _):
        for c in range(2):
            for d in range(2):
                for sub in range(2):
                    copy(c, d, t, sub).wait_send()
        return _

    lax.fori_loop(0, middle - 1, sent, 0)
    for c in range(2):
        copy(c, 0, middle - 1, 0).wait_send()
        copy(c, 1, middle - 1, 1).wait_send()
    for j in range(chunks // 2):
        at = slice(j * wide, (j + 1) * wide)
        pltpu.make_async_copy(y_s.at[:, at], y_hbm.at[:, at], y_sem.at[j]).wait()


def solution(mesh):
    n = mesh.shape["sp"]

    def step(x, gain, wq, wk, wv, wo):
        own, width = x.shape
        heads, kvh = wq.shape[1] // HEAD, wk.shape[1] // HEAD
        half = HEAD // 2
        cols = heads // kvh * own
        wide = 512
        chunks = wq.shape[1] // wide
        freq = (np.float32(THETA) ** (-np.arange(half, dtype=np.float32) / np.float32(half))).astype(np.float32)[None]
        hbm, vmem = pl.BlockSpec(memory_space=pl.ANY), pl.BlockSpec(memory_space=pltpu.VMEM)
        bf, f32 = jnp.bfloat16, jnp.float32
        dma = pltpu.SemaphoreType.DMA
        return pl.pallas_call(
            functools.partial(kernel, n),
            in_specs=[hbm, vmem, vmem, hbm, hbm, hbm, hbm],
            out_specs=hbm,
            out_shape=jax.ShapeDtypeStruct(x.shape, bf),
            scratch_shapes=[
                pltpu.VMEM((own, width), bf),
                pltpu.VMEM(wk.shape, bf),
                pltpu.VMEM(wv.shape, bf),
                pltpu.VMEM((chunks, width, wide), bf),
                pltpu.VMEM((own, width), bf),
                pltpu.VMEM((own, half), f32),
                pltpu.VMEM((own, half), f32),
                pltpu.VMEM((kvh, cols, HEAD), bf),
                pltpu.VMEM((n, kvh, 2, own, HEAD), bf),
                pltpu.VMEM((kvh, 1, cols), f32),
                pltpu.VMEM((kvh, HEAD + 8, cols), f32),
                pltpu.VMEM((own, heads * HEAD), bf),
                pltpu.VMEM((own, width), bf),
                dma,
                dma,
                dma,
                dma((chunks,)),
                dma((chunks // 2,)),
                dma((2, 2, n // 2, 2)),
                dma((2, 2, n // 2, 2)),
            ],
            compiler_params=pltpu.CompilerParams(collective_id=0, has_side_effects=True, vmem_limit_bytes=62 * 2**20),
        )(x, gain[None], freq, wq, wk, wv, wo)

    tokens, whole = P(("dp", "sp"), None), P(None, None)
    return jax.shard_map(
        step,
        mesh=mesh,
        in_specs=(tokens, P(None), whole, whole, whole, whole),
        out_specs=tokens,
        check_vma=False,
    )
```

```python
import functools
import math

import jax
import jax.numpy as jnp
import numpy as np
from jax import lax
from jax.experimental import pallas as pl
from jax.experimental.pallas import tpu as pltpu
from jax.sharding import PartitionSpec as P

HEAD = 256
THETA = 10000
LOG2E = 1.4426950408889634
HIDDEN = -2e30
STRIP = 512
PARTS = 2
MESH = pl.DeviceIdType.MESH


def dot(a, b, ca, cb):
    return lax.dot_general(a, b, (((ca,), (cb,)), ((), ())), preferred_element_type=jnp.float32)


def kernel(n, x_hbm, gain_ref, freq_ref, wq_hbm, wk_hbm, wv_hbm, wo_hbm, y_hbm, x_s, wk_s, wv_s, w_s, a_s, cos_s, sin_s, q_s, kv_s, top_s, mix_s, o_s, y_s,
           x_sem, wk_sem, wv_sem, w_sem, y_sem, send_sem, recv_sem):
    side = math.isqrt(n)
    own, width = x_s.shape
    half = HEAD // 2
    kvh, parts = kv_s.shape[1], kv_s.shape[2] // 2
    chunks, _, wide = w_s.shape
    heads = wq_hbm.shape[1] // HEAD
    group = heads // kvh
    cols = group * own
    me = lax.axis_index("sp")
    mx, my = me // side, me % side
    turn = (mx + my) % side
    place = (mx * side + turn, my * side + turn)

    def device(cycle, p):
        p = (p + n) % n
        major = p // side
        minor = (p % side + (side - 1) * major) % side
        return major * side + minor if cycle == 0 else minor * side + major

    neighbour = {(c, d): device(c, place[c] + (1 if d == 0 else -1)) for c in range(2) for d in range(2)}

    def source(c, d, t):
        return device(c, place[c] - t if d == 0 else place[c] + t)

    def copy(c, d, t, sub):
        block = kv_s.at[source(c, d, t), c, sub]
        return pltpu.make_async_remote_copy(src_ref=block, dst_ref=block, send_sem=send_sem.at[c, d, t, sub], recv_sem=recv_sem.at[c, d, t, sub],
                                            device_id={"sp": neighbour[c, d]}, device_id_type=MESH)

    def arrived(c, d, t, sub):
        block = kv_s.at[source(c, d, t), c, sub]
        pltpu.make_async_remote_copy(src_ref=block, dst_ref=block, send_sem=send_sem.at[c, d, t - 1, sub], recv_sem=recv_sem.at[c, d, t - 1, sub],
                                     device_id={"sp": neighbour[c, d]}, device_id_type=MESH).wait_recv()

    x_copy = pltpu.make_async_copy(x_hbm, x_s, x_sem)
    wk_copy = pltpu.make_async_copy(wk_hbm, wk_s, wk_sem)
    wv_copy = pltpu.make_async_copy(wv_hbm, wv_s, wv_sem)
    x_copy.start()
    wk_copy.start()
    wv_copy.start()

    barrier = pltpu.get_barrier_semaphore()
    for c in range(2):
        for d in range(2):
            pl.semaphore_signal(barrier, inc=1, device_id={"sp": neighbour[c, d]}, device_id_type=MESH)

    angle = (me * own + lax.broadcasted_iota(jnp.int32, (own, half), 0)).astype(jnp.float32) * freq_ref[...]
    cos_s[...] = jnp.cos(angle)
    sin_s[...] = jnp.sin(angle)

    def turned(t):
        a, b = t[:, :half], t[:, half:]
        return jnp.concatenate([a * cos_s[...] - b * sin_s[...], b * cos_s[...] + a * sin_s[...]], 1).astype(jnp.bfloat16)

    def rounded(t):
        return t.astype(jnp.bfloat16).astype(jnp.float32)

    x_copy.wait()
    rows = 32
    gain = gain_ref[...].astype(jnp.float32).reshape(1, width)

    def norm(i, _):
        at = pl.ds(pl.multiple_of(i * rows, rows), rows)
        t = x_s[at, :].astype(jnp.float32)
        scale = lax.rsqrt(jnp.mean(t * t, -1, keepdims=True) + 1e-6)
        a_s[at, :] = (t * scale * gain).astype(jnp.bfloat16)
        return _

    lax.fori_loop(0, own // rows, norm, 0)

    wk_copy.wait()
    keys = rounded(dot(a_s[...], wk_s[...], 1, 0))
    for c in range(kvh):
        kv_s[me, c, :parts] = turned(keys[:, c * HEAD : (c + 1) * HEAD]).reshape(parts, own // parts, HEAD)
    wv_copy.wait()

    def wq_copy(i):
        return pltpu.make_async_copy(wq_hbm.at[:, pl.ds(pl.multiple_of(i * wide, wide), wide)], w_s.at[i], w_sem.at[i])

    for i in range(chunks):
        wq_copy(i).start()
    pl.semaphore_wait(barrier, 4)
    for c in range(2):
        for d in range(2):
            for i in range(parts):
                copy(c, d, 0, i).start()
    values = dot(a_s[...], wv_s[...], 1, 0).astype(jnp.bfloat16)
    for c in range(kvh):
        kv_s[me, c, parts:] = values[:, c * HEAD : (c + 1) * HEAD].T.reshape(parts, HEAD // parts, own)
    per = wide // HEAD

    def project(i, _):
        wq_copy(i).wait()
        for j in range(per):
            t = rounded(dot(a_s[...], w_s[i, :, j * HEAD : (j + 1) * HEAD], 1, 0))
            h = i * per + j
            q_s[h // group, :, pl.ds(pl.multiple_of((h % group) * own, own), own)] = turned(t).T
        return _

    lax.fori_loop(0, 1, project, 0)
    for c in range(2):
        for d in range(2):
            for i in range(parts, 2 * parts):
                copy(c, d, 0, i).start()
    e = HEAD**-0.5 * LOG2E
    strips = range(0, cols, STRIP)
    ones = jnp.ones((8, own), jnp.bfloat16)

    def whole(slot, c, what):
        return kv_s[slot, c, what * parts : (what + 1) * parts].reshape(own, HEAD)

    def own_block(c):
        scores = [dot(whole(me, c, 0), q_s[c, :, at : at + STRIP], 1, 0) for at in strips]
        weights = []
        for at, s in zip(strips, scores):
            query = lax.broadcasted_iota(jnp.int32, (own, STRIP), 1) % own
            s = jnp.where(query >= lax.broadcasted_iota(jnp.int32, (own, STRIP), 0), s, HIDDEN)
            top = s.max(axis=0, keepdims=True)
            top_s[c, :, at : at + STRIP] = top
            weights.append(jnp.exp2((s - top) * e).astype(jnp.bfloat16))
        values = jnp.concatenate([whole(me, c, 1), ones], axis=0)
        for at, p in zip(strips, weights):
            mix_s[c, :, at : at + STRIP] = dot(values, p, 1, 0)

    def blocks(c, slots):
        seen = [slot < me for slot in slots]

        @pl.when(functools.reduce(jnp.logical_or, seen))
        def _():
            keys = jnp.concatenate([whole(slot, c, 0) for slot in slots], axis=0)
            scores = [dot(keys, q_s[c, :, at : at + STRIP], 1, 0) for at in strips]
            weights, keeps = [], []
            for at, s in zip(strips, scores):
                pieces = [s[i * own : (i + 1) * own] for i in range(len(slots))]
                old = top_s[c, :, at : at + STRIP]
                top = old
                for here, piece in zip(seen, pieces):
                    top = jnp.maximum(top, jnp.where(here, piece.max(axis=0, keepdims=True), HIDDEN))
                top_s[c, :, at : at + STRIP] = top
                p = [jnp.exp2((piece - jnp.where(here, top, -HIDDEN)) * e).astype(jnp.bfloat16) for here, piece in zip(seen, pieces)]
                weights.append(jnp.concatenate(p, axis=0))
                keeps.append(jnp.exp2((old - top) * e))
            values = jnp.concatenate([jnp.concatenate([whole(slot, c, 1), ones], axis=0) for slot in slots], axis=1)
            for at, p, keep in zip(strips, weights, keeps):
                mix_s[c, :, at : at + STRIP] = mix_s[c, :, at : at + STRIP] * keep + dot(values, p, 1, 0)

    def units(c, t):
        blocks(c, [source(c, d, t) for d in range(2)])

    def hand_on(t, what, last):
        for i in range(what * parts, (what + 1) * parts):
            for c in range(2):
                for d in range(2):
                    arrived(c, d, t, i)
                    if last is None or d == last:
                        copy(c, d, t, i).start()

    lax.fori_loop(1, chunks - 1, project, 0)
    hand_on(1, 0, None)
    lax.fori_loop(chunks - 1, chunks, project, 0)

    def wo_copy(i):
        r, j = i % 2, i // 2
        rows = w_s.shape[1]
        return pltpu.make_async_copy(wo_hbm.at[pl.ds(r * rows, rows), pl.ds(j * wide, wide)], w_s.at[i], w_sem.at[i])

    for i in range(chunks):
        wo_copy(i).start()
    for c in range(kvh):
        own_block(c)
    hand_on(1, 1, None)
    units(0, 1)
    middle = n // 2

    def step(t, _):
        hand_on(t, 0, None)
        units(1, t - 1)
        hand_on(t, 1, None)
        units(0, t)
        return _

    lax.fori_loop(2, middle - 1, step, 0)
    hand_on(middle - 1, 0, 0)
    units(1, middle - 2)
    hand_on(middle - 1, 1, 1)
    units(0, middle - 1)
    units(1, middle - 1)
    for c in range(2):
        for i in range(parts):
            arrived(c, 0, middle, i)
            arrived(c, 1, middle, parts + i)
        blocks(c, [source(c, 0, middle)])

    for c in range(kvh):
        for j in range(group):
            at = slice(j * own, (j + 1) * own)
            out = mix_s[c, :HEAD, at] * (1 / mix_s[c, HEAD : HEAD + 1, at])
            o_s[:, (c * group + j) * HEAD : (c * group + j + 1) * HEAD] = out.astype(jnp.bfloat16).T
    k = w_s.shape[1]
    for j in range(chunks // 2):
        at = slice(j * wide, (j + 1) * wide)
        wo_copy(2 * j).wait()
        wo_copy(2 * j + 1).wait()
        y = dot(o_s[:, :k], w_s[2 * j], 1, 0) + dot(o_s[:, k:], w_s[2 * j + 1], 1, 0)
        y_s[:, at] = (x_s[:, at].astype(jnp.float32) + y).astype(jnp.bfloat16)
        pltpu.make_async_copy(y_s.at[:, at], y_hbm.at[:, at], y_sem.at[j]).start()

    def sent(t, _):
        for c in range(2):
            for d in range(2):
                for sub in range(2 * parts):
                    copy(c, d, t, sub).wait_send()
        return _

    lax.fori_loop(0, middle - 1, sent, 0)
    for c in range(2):
        for i in range(parts):
            copy(c, 0, middle - 1, i).wait_send()
            copy(c, 1, middle - 1, parts + i).wait_send()
    for j in range(chunks // 2):
        at = slice(j * wide, (j + 1) * wide)
        pltpu.make_async_copy(y_s.at[:, at], y_hbm.at[:, at], y_sem.at[j]).wait()


def solution(mesh):
    n = mesh.shape["sp"]

    def step(x, gain, wq, wk, wv, wo):
        own, width = x.shape
        heads, kvh = wq.shape[1] // HEAD, wk.shape[1] // HEAD
        half = HEAD // 2
        cols = heads // kvh * own
        wide = 512
        chunks = wq.shape[1] // wide
        freq = (np.float32(THETA) ** (-np.arange(half, dtype=np.float32) / np.float32(half))).astype(np.float32)[None]
        hbm, vmem = pl.BlockSpec(memory_space=pl.ANY), pl.BlockSpec(memory_space=pltpu.VMEM)
        bf, f32 = jnp.bfloat16, jnp.float32
        dma = pltpu.SemaphoreType.DMA
        return pl.pallas_call(
            functools.partial(kernel, n),
            in_specs=[hbm, vmem, vmem, hbm, hbm, hbm, hbm],
            out_specs=hbm,
            out_shape=jax.ShapeDtypeStruct(x.shape, bf),
            scratch_shapes=[
                pltpu.VMEM((own, width), bf),
                pltpu.VMEM(wk.shape, bf),
                pltpu.VMEM(wv.shape, bf),
                pltpu.VMEM((chunks, width, wide), bf),
                pltpu.VMEM((own, width), bf),
                pltpu.VMEM((own, half), f32),
                pltpu.VMEM((own, half), f32),
                pltpu.VMEM((kvh, HEAD, cols), bf),
                pltpu.VMEM((n, kvh, 2 * PARTS, own // PARTS, HEAD), bf),
                pltpu.VMEM((kvh, 1, cols), f32),
                pltpu.VMEM((kvh, HEAD + 8, cols), f32),
                pltpu.VMEM((own, heads * HEAD), bf),
                pltpu.VMEM((own, width), bf),
                dma,
                dma,
                dma,
                dma((chunks,)),
                dma((chunks // 2,)),
                dma((2, 2, n // 2, 2 * PARTS)),
                dma((2, 2, n // 2, 2 * PARTS)),
            ],
            compiler_params=pltpu.CompilerParams(collective_id=0, has_side_effects=True, vmem_limit_bytes=62 * 2**20),
        )(x, gain, freq, wq, wk, wv, wo)

    tokens, whole = P(("dp", "sp"), None), P(None, None)
    return jax.shard_map(
        step,
        mesh=mesh,
        in_specs=(tokens, P(None), whole, whole, whole, whole),
        out_specs=tokens,
        check_vma=False,
    )
```

```python
import functools
import math

import jax
import jax.numpy as jnp
import numpy as np
from jax import lax
from jax.experimental import pallas as pl
from jax.experimental.pallas import tpu as pltpu
from jax.sharding import PartitionSpec as P

HEAD = 256
THETA = 10000
LOG2E = 1.4426950408889634
HIDDEN = -2e30
STRIP = 512
PARTS = 2
MESH = pl.DeviceIdType.MESH


def dot(a, b, ca, cb):
    return lax.dot_general(a, b, (((ca,), (cb,)), ((), ())), preferred_element_type=jnp.float32)


def kernel(n, x_hbm, gain_ref, freq_ref, wq_hbm, wk_hbm, wv_hbm, wo_hbm, y_hbm, x_s, wk_s, wv_s, w_s, a_s, cos_s, sin_s, q_s, kv_s, top_s, mix_s, o_s,
           x_sem, wk_sem, wv_sem, w_sem, send_sem, recv_sem):
    side = math.isqrt(n)
    own, width = x_s.shape
    half = HEAD // 2
    kvh, parts = kv_s.shape[1], kv_s.shape[2] // 2
    chunks, _, wide = w_s.shape
    heads = wq_hbm.shape[1] // HEAD
    group = heads // kvh
    cols = group * own
    me = lax.axis_index("sp")
    mx, my = me // side, me % side
    turn = (mx + my) % side
    place = (mx * side + turn, my * side + turn)

    def device(cycle, p):
        p = (p + n) % n
        major = p // side
        minor = (p % side + (side - 1) * major) % side
        return major * side + minor if cycle == 0 else minor * side + major

    neighbour = {(c, d): device(c, place[c] + (1 if d == 0 else -1)) for c in range(2) for d in range(2)}

    def source(c, d, t):
        return device(c, place[c] - t if d == 0 else place[c] + t)

    def copy(c, d, t, sub):
        block = kv_s.at[source(c, d, t), c, sub]
        return pltpu.make_async_remote_copy(src_ref=block, dst_ref=block, send_sem=send_sem, recv_sem=recv_sem.at[c, t, sub],
                                            device_id={"sp": neighbour[c, d]}, device_id_type=MESH)

    def arrived(c, t, sub, count):
        size = kv_s.at[pl.ds(0, count), c, sub]
        pltpu.make_async_copy(size, size, recv_sem.at[c, t - 1, sub]).wait()

    x_copy = pltpu.make_async_copy(x_hbm, x_s, x_sem)
    wk_copy = pltpu.make_async_copy(wk_hbm, wk_s, wk_sem)
    wv_copy = pltpu.make_async_copy(wv_hbm, wv_s, wv_sem)
    x_copy.start()

    barrier = pltpu.get_barrier_semaphore()
    for c in range(2):
        for d in range(2):
            pl.semaphore_signal(barrier, inc=1, device_id={"sp": neighbour[c, d]}, device_id_type=MESH)

    wk_copy.start()
    wv_copy.start()
    angle = (me * own + lax.broadcasted_iota(jnp.int32, (own, half), 0)).astype(jnp.float32) * freq_ref[...]
    cos_s[...] = jnp.cos(angle)
    sin_s[...] = jnp.sin(angle)

    def turned(t):
        a, b = t[:, :half], t[:, half:]
        return jnp.concatenate([a * cos_s[...] - b * sin_s[...], b * cos_s[...] + a * sin_s[...]], 1).astype(jnp.bfloat16)

    def rounded(t):
        return t.astype(jnp.bfloat16).astype(jnp.float32)

    x_copy.wait()
    rows = 128
    gain = gain_ref[...].astype(jnp.float32).reshape(1, width)

    def norm(i, _):
        at = pl.ds(pl.multiple_of(i * rows, rows), rows)
        t = x_s[at, :].astype(jnp.float32)
        scale = lax.rsqrt(jnp.mean(t * t, -1, keepdims=True) + 1e-6)
        a_s[at, :] = (t * scale * gain).astype(jnp.bfloat16)
        return _

    lax.fori_loop(0, own // rows, norm, 0)

    wk_copy.wait()
    keys = rounded(dot(a_s[...], wk_s[...], 1, 0))
    for c in range(kvh):
        kv_s[me, c, :parts] = turned(keys[:, c * HEAD : (c + 1) * HEAD]).reshape(parts, own // parts, HEAD)
    wv_copy.wait()

    def wq_copy(i):
        return pltpu.make_async_copy(wq_hbm.at[:, pl.ds(pl.multiple_of(i * wide, wide), wide)], w_s.at[i], w_sem.at[i])

    for i in range(chunks):
        wq_copy(i).start()
    pl.semaphore_wait(barrier, 4)
    for c in range(2):
        for d in range(2):
            for i in range(parts):
                copy(c, d, 0, i).start()
    values = dot(a_s[...], wv_s[...], 1, 0).astype(jnp.bfloat16)
    for c in range(kvh):
        kv_s[me, c, parts:] = values[:, c * HEAD : (c + 1) * HEAD].T.reshape(parts, HEAD // parts, own)
    for c in range(2):
        for d in range(2):
            for i in range(parts, 2 * parts):
                copy(c, d, 0, i).start()
    per = wide // HEAD

    def project(i, _):
        wq_copy(i).wait()
        for j in range(per):
            t = rounded(dot(a_s[...], w_s[i, :, j * HEAD : (j + 1) * HEAD], 1, 0))
            h = i * per + j
            q_s[h // group, :, pl.ds(pl.multiple_of((h % group) * own, own), own)] = turned(t).T
        return _

    e = HEAD**-0.5 * LOG2E
    strips = range(0, cols, STRIP)
    ones = jnp.ones((8, own), jnp.bfloat16)

    def whole(slot, c, what):
        return kv_s[slot, c, what * parts : (what + 1) * parts].reshape(own, HEAD)

    def own_block(c):
        scores = [dot(whole(me, c, 0), q_s[c, :, at : at + STRIP], 1, 0) for at in strips]
        weights = []
        for at, s in zip(strips, scores):
            query = lax.broadcasted_iota(jnp.int32, (own, STRIP), 1) % own
            s = jnp.where(query >= lax.broadcasted_iota(jnp.int32, (own, STRIP), 0), s, HIDDEN)
            top = s.max(axis=0, keepdims=True)
            top_s[c, :, at : at + STRIP] = top
            weights.append(jnp.exp2((s - top) * e).astype(jnp.bfloat16))
        values = jnp.concatenate([whole(me, c, 1), ones], axis=0)
        for at, p in zip(strips, weights):
            mix_s[c, :, at : at + STRIP] = dot(values, p, 1, 0)

    def blocks(c, slots):
        seen = [slot < me for slot in slots]

        @pl.when(functools.reduce(jnp.logical_or, seen))
        def _():
            keys = jnp.concatenate([whole(slot, c, 0) for slot in slots], axis=0)
            scores = [dot(keys, q_s[c, :, at : at + STRIP], 1, 0) for at in strips]
            weights, keeps = [], []
            for at, s in zip(strips, scores):
                pieces = [s[i * own : (i + 1) * own] for i in range(len(slots))]
                old = top_s[c, :, at : at + STRIP]
                top = old
                for here, piece in zip(seen, pieces):
                    top = jnp.maximum(top, jnp.where(here, piece.max(axis=0, keepdims=True), HIDDEN))
                top_s[c, :, at : at + STRIP] = top
                p = [jnp.exp2((piece - jnp.where(here, top, -HIDDEN)) * e).astype(jnp.bfloat16) for here, piece in zip(seen, pieces)]
                weights.append(jnp.concatenate(p, axis=0))
                keeps.append(jnp.exp2((old - top) * e))
            values = jnp.concatenate([jnp.concatenate([whole(slot, c, 1), ones], axis=0) for slot in slots], axis=1)
            for at, p, keep in zip(strips, weights, keeps):
                mix_s[c, :, at : at + STRIP] = mix_s[c, :, at : at + STRIP] * keep + dot(values, p, 1, 0)

    def units(c, t):
        blocks(c, [source(c, d, t) for d in range(2)])

    def hand_on(t, what, last):
        for i in range(what * parts, (what + 1) * parts):
            for c in range(2):
                arrived(c, t, i, 2)
                for d in range(2):
                    if last is None or d == last:
                        copy(c, d, t, i).start()

    lax.fori_loop(0, chunks - 1, project, 0)
    hand_on(1, 0, None)
    lax.fori_loop(chunks - 1, chunks, project, 0)

    def wo_copy(i):
        r, j = i % 2, i // 2
        rows = w_s.shape[1]
        return pltpu.make_async_copy(wo_hbm.at[pl.ds(r * rows, rows), pl.ds(j * wide, wide)], w_s.at[i], w_sem.at[i])

    for i in range(chunks):
        wo_copy(i).start()
    for c in range(kvh):
        own_block(c)
    hand_on(1, 1, None)
    units(0, 1)
    middle = n // 2

    def step(t, _):
        hand_on(t, 0, None)
        units(1, t - 1)
        hand_on(t, 1, None)
        units(0, t)
        return _

    lax.fori_loop(2, middle - 1, step, 0)
    hand_on(middle - 1, 0, 0)
    units(1, middle - 2)
    hand_on(middle - 1, 1, 1)
    units(0, middle - 1)
    units(1, middle - 1)
    for c in range(2):
        for i in range(parts):
            arrived(c, middle, i, 1)
            arrived(c, middle, parts + i, 1)
        blocks(c, [source(c, 0, middle)])

    for c in range(kvh):
        for j in range(group):
            at = slice(j * own, (j + 1) * own)
            out = mix_s[c, :HEAD, at] * (1 / mix_s[c, HEAD : HEAD + 1, at])
            o_s[:, (c * group + j) * HEAD : (c * group + j + 1) * HEAD] = out.astype(jnp.bfloat16).T
    k = w_s.shape[1]
    for j in range(chunks // 2):
        at = slice(j * wide, (j + 1) * wide)
        wo_copy(2 * j).wait()
        wo_copy(2 * j + 1).wait()
        y = dot(o_s[:, :k], w_s[2 * j], 1, 0) + dot(o_s[:, k:], w_s[2 * j + 1], 1, 0)
        y_hbm[:, at] = (x_s[:, at].astype(jnp.float32) + y).astype(jnp.bfloat16)

    everything = kv_s.at[pl.ds(0, n - 1)]
    pltpu.make_async_copy(everything, everything, send_sem).wait()


def solution(mesh):
    n = mesh.shape["sp"]

    def step(x, gain, wq, wk, wv, wo):
        own, width = x.shape
        heads, kvh = wq.shape[1] // HEAD, wk.shape[1] // HEAD
        half = HEAD // 2
        cols = heads // kvh * own
        wide = 512
        chunks = wq.shape[1] // wide
        freq = (np.float32(THETA) ** (-np.arange(half, dtype=np.float32) / np.float32(half))).astype(np.float32)[None]
        hbm, vmem = pl.BlockSpec(memory_space=pltpu.HBM), pl.BlockSpec(memory_space=pltpu.VMEM)
        bf, f32 = jnp.bfloat16, jnp.float32
        dma = pltpu.SemaphoreType.DMA
        return pl.pallas_call(
            functools.partial(kernel, n),
            in_specs=[hbm, vmem, vmem, hbm, hbm, hbm, hbm],
            out_specs=vmem,
            out_shape=pltpu.VMEM(x.shape, bf),
            scratch_shapes=[
                pltpu.VMEM((own, width), bf),
                pltpu.VMEM(wk.shape, bf),
                pltpu.VMEM(wv.shape, bf),
                pltpu.VMEM((chunks, width, wide), bf),
                pltpu.VMEM((own, width), bf),
                pltpu.VMEM((own, half), f32),
                pltpu.VMEM((own, half), f32),
                pltpu.VMEM((kvh, HEAD, cols), bf),
                pltpu.VMEM((n, kvh, 2 * PARTS, own // PARTS, HEAD), bf),
                pltpu.VMEM((kvh, 1, cols), f32),
                pltpu.VMEM((kvh, HEAD + 8, cols), f32),
                pltpu.VMEM((own, heads * HEAD), bf),
                dma,
                dma,
                dma,
                dma((chunks,)),
                dma,
                dma((2, n // 2, 2 * PARTS)),
            ],
            compiler_params=pltpu.CompilerParams(collective_id=0, has_side_effects=True, vmem_limit_bytes=56 * 2**20),
        )(x, gain, freq, wq, wk, wv, wo)

    tokens, whole = P(("dp", "sp"), None), P(None, None)
    return jax.shard_map(
        step,
        mesh=mesh,
        in_specs=(tokens, P(None), whole, whole, whole, whole),
        out_specs=tokens,
        check_vma=False,
    )
```
